256 devices in a mesh: site: 64 (over z_hi, x, y, core), vec: 4 (over z_lo).
Axes of the slice: x: 4, y: 4, z: 8 (z_hi: 2, z_lo: 4; z = z_hi * 4 + z_lo), core: 2. Of those that a mesh axis runs over, the one named last changes fastest.
Arguments:
- vector_signs: int32 [64, 1024, 2048], P('vec', 'site'), may hold values from 0 to 1
- disorder: int32 [1024, 2048], P('site'), may hold values from 0 to 7
- bond_types: int32 [2, 1024, 2048], P(None, 'site'), may hold values from 0 to 3
- onsite_table: float32 [8], replicated, may hold values from -2 to 2
- hop_table: float32 [4], replicated, may hold values from 0.5 to 1.5
Outputs:
- moments: float32 [4, 4, 16, 16], replicated
The draws below stay inside these ranges and needn't reach their ends.
All inputs are finite; a program needn't handle non-finite values.
Results may differ from the reference program's by a relative error of at most 0.000075.
Values sent between devices are 32-bit elements; how exact they have to be, the bound alone decides.
A program may use at most 128 MiB of HBM per device.

```python
import jax
import jax.numpy as jnp
from jax import lax

R = 16
ORDERS = 4
CLASSES = 8
BONDS = 4
COLS = 2048
NY = 1024
SITES = 2097152
VECS = 64
N_VEC = 4


def plant(drawn, stream_key, smallest, high):
    dims = drawn.shape
    index_at = [jax.random.randint(jax.random.fold_in(stream_key, axis), (), 0, dims[axis]) for axis in range(len(dims))]
    drawn = drawn.at[tuple(index_at)].set(smallest)
    longest = dims.index(max(dims))
    index_at[longest] = (index_at[longest] + 1) % dims[longest]
    return drawn.at[tuple(index_at)].set(high)


def setup_inputs(seed: int = 0) -> dict:
    key_of = jax.random.split(jax.random.key(seed), 6)
    return {
        "vector_signs": plant(jax.random.randint(key_of[0], (VECS, NY, COLS), 0, 2), jax.random.fold_in(key_of[0], 1), 0, 1).astype(jnp.int32),
        "disorder": plant(jax.random.randint(key_of[1], (NY, COLS), 0, CLASSES), jax.random.fold_in(key_of[1], 1), 0, CLASSES - 1).astype(jnp.int32),
        "bond_types": plant(jax.random.randint(key_of[2], (2, NY, COLS), 0, BONDS), jax.random.fold_in(key_of[2], 1), 0, BONDS - 1).astype(jnp.int32),
        "onsite_table": jnp.clip(jax.random.uniform(key_of[3], (CLASSES,), jnp.float32, -2.0, 2.0), -2.0, 2.0),
        "hop_table": jnp.clip(jax.random.uniform(key_of[4], (BONDS,), jnp.float32, 0.5, 1.5), 0.5, 1.5),
    }


spectral_bound = 8.5


def lookup(codes, table):
    result = jnp.zeros(codes.shape, jnp.float32)
    for k in range(table.shape[0]):
        result = jnp.where(codes == k, table[k], result)
    return result


def hamiltonian(window, fields, bonds_y):
    onsite, hop_x = fields
    center = window[..., 1:-1, :]
    upper = window[..., 2:, :]
    lower = window[..., :-2, :]
    column_sum = hop_x * jnp.roll(center, -1, -1) + jnp.roll(hop_x * center, 1, -1)
    total = column_sum + bonds_y[1:] * upper + bonds_y[:-1] * lower
    return (onsite * center - total) * (1.0 / spectral_bound)


def velocity(window, fields, bonds_y):
    upper = window[..., 2:, :]
    lower = window[..., :-2, :]
    return bonds_y[1:] * upper - bonds_y[:-1] * lower


def wrapped(stack):
    return jnp.concatenate([stack[..., -1:, :], stack, stack[..., :1, :]], axis=-2)


def reference(vector_signs, disorder, bond_types, onsite_table, hop_table):
    onsite = lookup(disorder, onsite_table)
    hop_x = lookup(bond_types[0], hop_table)
    hop_y = lookup(bond_types[1], hop_table)
    bonds_y = jnp.concatenate([hop_y[-1:], hop_y], axis=0)
    fields = (onsite, hop_x)
    groups = vector_signs.reshape(N_VEC, R, vector_signs.shape[1], vector_signs.shape[2])

    def one_group(group_signs):
        start = (2 * group_signs - 1).astype(jnp.float32)
        padded = wrapped(start)
        left_zero = velocity(padded, (), bonds_y)
        right_zero = start
        right_one = hamiltonian(padded, fields, bonds_y)
        drift_zero = left_zero
        stack = jnp.stack([left_zero, right_one])
        padded = wrapped(stack)
        applied = hamiltonian(padded, fields, bonds_y)
        left_one = applied[0]
        right_two = 2.0 * applied[1] - right_zero
        drift_one = velocity(padded[1], (), bonds_y)
        stack = jnp.stack([left_one, right_two])
        padded = wrapped(stack)
        applied = hamiltonian(padded, fields, bonds_y)
        left_two = 2.0 * applied[0] - left_zero
        right_three = 2.0 * applied[1] - right_one
        drift_two = velocity(padded[1], (), bonds_y)
        stack = jnp.stack([left_two, right_three])
        padded = wrapped(stack)
        left_three = 2.0 * hamiltonian(padded[0], fields, bonds_y) - left_one
        drift_three = velocity(padded[1], (), bonds_y)
        lefts = jnp.stack([left_zero, left_one, left_two, left_three]).reshape(ORDERS * R, -1)
        drifts = jnp.stack([drift_zero, drift_one, drift_two, drift_three]).reshape(ORDERS * R, -1)
        return lax.dot_general(lefts, drifts, (((1,), (1,)), ((), ())), precision=lax.Precision.HIGHEST, preferred_element_type=jnp.float32)

    partials = lax.map(one_group, groups)
    summed = jnp.sum(partials, axis=0)
    shaped = summed.reshape(ORDERS, R, ORDERS, R).transpose(0, 2, 1, 3)
    return shaped * (-1.0 / (SITES * N_VEC))
```

```python
import functools

import jax
import jax.numpy as jnp
from jax import lax
from jax.experimental import pallas as pl
from jax.experimental.pallas import tpu as pltpu
from jax.sharding import PartitionSpec as P

MESH = pl.DeviceIdType.MESH
DEPTH = 4
SPLIT = (2, 4, 4, 2)
spectral_bound = 8.5
scale = 2.0 / spectral_bound


def rolled(v, shift):
    return pltpu.roll(v, shift % v.shape[1], 1)


def lookup(codes, table, count, factor):
    result = jnp.zeros(codes.shape, jnp.float32)
    for k in range(count):
        result = jnp.where(codes == k, table[k] * factor, result)
    return result


def kernel(
    dims,
    signs,
    disorder,
    bonds,
    onsite_table,
    hop_table,
    out,
    codes,
    fields,
    raw,
    base,
    right_1,
    right_2,
    right_3,
    left_0,
    left_1,
    left_2,
    lefts,
    drifts,
    acc,
    packed,
    core_in,
    y_buf,
    x_buf,
    z_buf,
    final,
    row_sem,
    code_sem,
    row_send,
    row_recv,
    code_send,
    code_recv,
    red_send,
    red_recv,
):
    n_hi, n_x, n_y, n_core, n_lo = dims
    n_site = n_hi * n_x * n_y * n_core
    n_z = n_hi * n_lo
    rows = signs.shape[1]
    total = rows + 2 * DEPTH
    cols = signs.shape[2]
    half_rows = 8
    site = lax.axis_index("site")
    vec = lax.axis_index("vec")
    core = lax.rem(site, n_core)
    y = lax.rem(site // n_core, n_y)
    x = lax.rem(site // (n_core * n_y), n_x)
    z = (site // (n_core * n_y * n_x)) * n_lo + vec

    def device(xx, yy, zz):
        return (
            (zz // n_lo) * (n_x * n_y * n_core) + xx * (n_y * n_core) + yy * n_core + core,
            lax.rem(zz, n_lo),
        )

    partner = (site + 1 - 2 * core, vec)
    across = (lax.rem(site + n_site + 2 * core - 1, n_site), vec)
    y_peers = [device(x, lax.rem(y + k, n_y), z) for k in range(1, n_y)]
    x_peers = [device(lax.rem(x + k, n_x), y, z) for k in range(1, n_x)]
    z_peers = [device(x, y, lax.rem(z + k, n_z)) for k in range(1, n_z)]

    barrier = pltpu.get_barrier_semaphore()
    everyone = [partner, across, *y_peers, *x_peers, *z_peers]
    for peer in everyone:
        pl.semaphore_signal(barrier, inc=1, device_id=peer, device_id_type=MESH)

    def mine(k):
        return pltpu.make_async_copy(signs.at[:, k], raw.at[DEPTH + k], row_sem.at[k])

    def far_row(i):
        return core * (rows - 1 - i) + (1 - core) * i

    def near_row(i):
        return (1 - core) * (rows - 1 - i) + core * i

    for i in range(DEPTH):
        mine(near_row(i)).start()
    own_codes = [
        pltpu.make_async_copy(src, codes.at[j, pl.ds(0, rows)], code_sem.at[j])
        for j, src in enumerate((disorder, bonds.at[0], bonds.at[1]))
    ]
    for copy in own_codes:
        copy.start()
    for i in range(DEPTH):
        mine(far_row(i)).start()
    for i in range(DEPTH, rows - DEPTH):
        mine(i).start()

    def send_row(side, i):
        own = near_row(i) if side == 0 else far_row(i)
        flag = core if side == 0 else 1 - core
        there = flag * (DEPTH + rows + i) + (1 - flag) * (DEPTH - 1 - i)
        return pltpu.make_async_remote_copy(
            src_ref=raw.at[DEPTH + own],
            dst_ref=raw.at[there],
            send_sem=row_send.at[side, i],
            recv_sem=row_recv.at[side, i],
            device_id=partner if side == 0 else across,
            device_id_type=MESH,
        )

    def send_codes(side, upward, j):
        src = rows - DEPTH if upward else 0
        dst = rows + DEPTH if upward else rows
        return pltpu.make_async_remote_copy(
            src_ref=codes.at[j, pl.ds(src, DEPTH)],
            dst_ref=codes.at[j, pl.ds(dst, DEPTH)],
            send_sem=code_send.at[side, j],
            recv_sem=code_recv.at[side, j],
            device_id=partner if side == 0 else across,
            device_id_type=MESH,
        )

    pl.semaphore_wait(barrier, len(everyone))
    for i in range(DEPTH):
        mine(near_row(i)).wait()
        send_row(0, i).start()
    for copy in own_codes:
        copy.wait()

    @pl.when(core == 1)
    def _():
        for j in range(3):
            send_codes(0, False, j).start()
            send_codes(1, True, j).start()

    @pl.when(core == 0)
    def _():
        for j in range(3):
            send_codes(0, True, j).start()
            send_codes(1, False, j).start()

    for i in range(DEPTH):
        mine(far_row(i)).wait()
        send_row(1, i).start()
    for i in range(DEPTH, rows - DEPTH):
        mine(i).wait()

    def decode(start, size):
        at = pl.ds(start, size)
        fields[0, at, :] = lookup(codes[0, at, :], onsite_table, onsite_table.shape[0], scale)
        fields[1, at, :] = lookup(codes[1, at, :], hop_table, hop_table.shape[0], -scale)
        fields[2, at, :] = lookup(codes[2, at, :], hop_table, hop_table.shape[0], -scale)

    def decode_side(side):
        upper = side == 1
        for j in range(3):
            send_codes(side, True, j).wait_recv()

        @pl.when(core == 1)
        def _():
            decode(rows if upper else rows + DEPTH, DEPTH)

        @pl.when(core == 0)
        def _():
            decode(rows + DEPTH if upper else rows, DEPTH)

    for start in range(0, rows, 8):
        decode(start, 8)
    decode_side(0)
    for i in range(DEPTH):
        send_row(0, i).wait_recv()

    def natural(s):
        return core * s + (1 - core) * (total - 1 - s)

    def place(n):
        return lax.rem(n + total - DEPTH, total)

    def site_field(j, s):
        return jnp.broadcast_to(fields[j, pl.ds(place(natural(s)), 1), :], (half_rows, cols))

    def bond(s):
        n = core * s + (1 - core) * (total - 2 - s)
        return jnp.broadcast_to(fields[2, pl.ds(place(n), 1), :], (half_rows, cols))

    def keep(stack, order, s, h, v):
        high = v.astype(jnp.bfloat16).astype(jnp.float32)
        both = jnp.concatenate([high, v - high], axis=0).astype(jnp.bfloat16)
        at = pl.ds(pl.multiple_of(order * 32 + h * 16, 16), 16)
        if stack is None:
            lefts[lax.rem(s, 8), at, :] = both
            drifts[lax.rem(s, 8), at, :] = both
        else:
            stack[lax.rem(s, 8), at, :] = both

    def columns(v, s):
        hop = site_field(1, s)
        return site_field(0, s) * v + hop * rolled(v, -1) + rolled(hop * v, 1)

    def load_base(t, h):
        codes_now = raw[natural(t), pl.ds(pl.multiple_of(h * 8, 8), 8), :]
        value = jnp.where(codes_now == 1, 1.0, -1.0).astype(jnp.float32)
        base[t, h] = value
        return value

    def advance(u, levels):
        t = u // 2
        h = lax.rem(u, 2)
        ahead = load_base(t, h)
        if levels >= 1:
            s = t - 1
            forth, back = bond(s) * ahead, bond(s - 1) * base[s - 1, h]
            left_new = forth - back
            left_0[s, h] = left_new
            keep(None, 0, s, h, left_new)
            right_new = columns(base[s, h], s) + (forth + back)
            right_1[s, h] = right_new
        if levels >= 2:
            s = t - 2
            up, down = bond(s), bond(s - 1)
            forth, back = up * right_new, down * right_1[s - 1, h]
            keep(drifts, 1, s, h, forth - back)
            twice = base[s, h]
            right_new = columns(right_1[s, h], s) + (forth + back) - (twice + twice)
            right_2[s, h] = right_new
            left_new = columns(left_0[s, h], s) + (up * left_new + down * left_0[s - 1, h])
            left_1[s, h] = left_new
            keep(lefts, 1, s, h, left_new)
        if levels >= 3:
            s = t - 3
            up, down = bond(s), bond(s - 1)
            forth, back = up * right_new, down * right_2[s - 1, h]
            keep(drifts, 2, s, h, forth - back)
            right_new = columns(right_2[s, h], s) + (forth + back) - right_1[s, h]
            right_3[s, h] = right_new
            twice = left_0[s, h]
            left_new = columns(left_1[s, h], s) + (up * left_new + down * left_1[s - 1, h]) - (twice + twice)
            left_2[s, h] = left_new
            keep(lefts, 2, s, h, left_new)
        if levels >= 4:
            s = t - 4
            up, down = bond(s), bond(s - 1)
            keep(drifts, 3, s, h, up * right_new - down * right_3[s - 1, h])
            left_new = columns(left_2[s, h], s) + (up * left_new + down * left_2[s - 1, h]) - left_1[s, h]
            keep(lefts, 3, s, h, left_new)

    width = cols // 2

    def multiply(s, h):
        slot = lax.rem(s, 8)
        at = pl.ds(pl.multiple_of(h * width, 128), width)
        acc[...] += lax.dot_general(
            lefts[slot, :, at],
            drifts[slot, :, at],
            (((1,), (1,)), ((), ())),
            preferred_element_type=jnp.float32,
        )

    for levels in range(4):
        first = 0 if levels == 0 else 2 * levels

        def warm(u, carry, levels=levels):
            advance(u, levels)
            return carry

        lax.fori_loop(2 * first, 2 * (2 * levels + 2), warm, 0)

    first_full = 2 * DEPTH

    def full(u, carry):
        t = u // 2

        @pl.when(u == 2 * (rows + DEPTH))
        def _():
            decode_side(1)

        @pl.when(jnp.logical_and(t >= rows + DEPTH, lax.rem(u, 2) == 0))
        def _():
            i = t - (rows + DEPTH)
            pltpu.make_async_copy(signs.at[:, 0], raw.at[0], row_recv.at[1, i]).wait()

        multiply(t - 5, lax.rem(u, 2))

        @pl.when(u == 2 * first_full + 1)
        def _():
            acc[...] = jnp.zeros_like(acc)

        advance(u, 4)
        return carry

    lax.fori_loop(2 * first_full, 2 * total, full, 0)
    for h in range(2):
        multiply(total - 1 - DEPTH, h)

    whole = jnp.concatenate([acc[16 * b : 16 * b + 8, :] + acc[16 * b + 8 : 16 * b + 16, :] for b in range(8)], axis=0)
    whole = whole + rolled(whole, -8)
    lane = lax.broadcasted_iota(jnp.int32, (32, 128), 1)
    packed[...] = jnp.where((lane // 8) % 2 == 0, whole[:32], rolled(whole[32:], 8)).reshape(2, 16, 128)

    def send(src, dst, k, peer):
        return pltpu.make_async_remote_copy(
            src_ref=src, dst_ref=dst, send_sem=red_send.at[k], recv_sem=red_recv.at[k], device_id=peer, device_id_type=MESH
        )

    first = send(packed.at[1 - core], core_in, 0, partner)
    first.start()
    first.wait_recv()
    value = packed[core] + core_in[...]
    waits = [first]
    start = 1
    for buf, place_now, peers, size in ((y_buf, y, y_peers, n_y), (x_buf, x, x_peers, n_x), (z_buf, z, z_peers, n_z)):
        buf[place_now] = value
        for k, peer in enumerate(peers):
            copy = pltpu.make_async_remote_copy(
                src_ref=buf.at[place_now],
                dst_ref=buf.at[place_now],
                send_sem=red_send.at[start + k],
                recv_sem=red_recv.at[start + k],
                device_id=peer,
                device_id_type=MESH,
            )
            copy.start()
            waits.append(copy)
        for k in range(size - 1):
            waits[start + k].wait_recv()
        value = buf[0]
        for k in range(1, size):
            value = value + buf[k]
        start += size - 1
    final[core] = value
    last = send(final.at[core], final.at[core], start, partner)
    last.start()
    last.wait_recv()
    waits.append(last)

    done = final[...].reshape(32, 128)
    lane = lax.broadcasted_iota(jnp.int32, (16, 128), 1)
    per_site = -1.0 / (n_site * rows * cols * n_lo) / (scale * scale)
    for p in range(4):
        strip = done[(p % 2) * 16 : (p % 2) * 16 + 16]
        for q in range(4):
            at = q * 32 + (p // 2) * 8
            block = jnp.where(lane < 8, rolled(strip, -at), rolled(strip, -at - 8))
            factor = per_site * (0.5 if p else 1.0) * (0.5 if q else 1.0)
            out[p, q] = block[:, :16] * factor

    for copy in waits:
        copy.wait_send()
    for side in range(2):
        for i in range(DEPTH):
            send_row(side, i).wait_send()
        for j in range(3):
            send_codes(side, True, j).wait_send()


def solution(mesh):
    n_hi, n_x, n_y, n_core = SPLIT
    n_lo = mesh.shape["vec"]
    dims = (mesh.shape["site"] // (n_x * n_y * n_core), n_x, n_y, n_core, n_lo)

    def shards(vector_signs, disorder, bond_types, onsite_table, hop_table):
        width, rows, cols = vector_signs.shape
        total = rows + 2 * DEPTH
        n_red = 2 + (n_y - 1) + (n_x - 1) + (dims[0] * n_lo - 1)
        full = pltpu.VMEM((total, 2, 8, cols), jnp.float32)
        anywhere = pl.BlockSpec(memory_space=pl.ANY)
        scalars = pl.BlockSpec(memory_space=pltpu.SMEM)
        return pl.pallas_call(
            functools.partial(kernel, dims),
            out_shape=jax.ShapeDtypeStruct((4, 4, width, width), jnp.float32),
            in_specs=[anywhere, anywhere, anywhere, scalars, scalars],
            out_specs=pl.BlockSpec(memory_space=pltpu.VMEM),
            scratch_shapes=[
                pltpu.VMEM((3, total, cols), jnp.int32),
                pltpu.VMEM((3, total, cols), jnp.float32),
                pltpu.VMEM((total, width, cols), jnp.int32),
                full,
                full,
                full,
                full,
                full,
                full,
                full,
                pltpu.VMEM((8, 128, cols), jnp.bfloat16),
                pltpu.VMEM((8, 128, cols), jnp.bfloat16),
                pltpu.VMEM((128, 128), jnp.float32),
                pltpu.VMEM((2, 16, 128), jnp.float32),
                pltpu.VMEM((16, 128), jnp.float32),
                pltpu.VMEM((n_y, 16, 128), jnp.float32),
                pltpu.VMEM((n_x, 16, 128), jnp.float32),
                pltpu.VMEM((dims[0] * n_lo, 16, 128), jnp.float32),
                pltpu.VMEM((2, 16, 128), jnp.float32),
                pltpu.SemaphoreType.DMA((rows,)),
                pltpu.SemaphoreType.DMA((3,)),
                pltpu.SemaphoreType.DMA((2, DEPTH)),
                pltpu.SemaphoreType.DMA((2, DEPTH)),
                pltpu.SemaphoreType.DMA((2, 3)),
                pltpu.SemaphoreType.DMA((2, 3)),
                pltpu.SemaphoreType.DMA((n_red,)),
                pltpu.SemaphoreType.DMA((n_red,)),
            ],
            compiler_params=pltpu.CompilerParams(
                collective_id=0, has_side_effects=True, vmem_limit_bytes=60 * 1024 * 1024
            ),
        )(vector_signs, disorder, bond_types, onsite_table, hop_table)

    return jax.shard_map(
        shards,
        mesh=mesh,
        in_specs=(P("vec", "site", None), P("site", None), P(None, "site", None), P(), P()),
        out_specs=P(),
        check_vma=False,
    )
```

```python
import functools

import jax
import jax.numpy as jnp
from jax import lax
from jax.experimental import pallas as pl
from jax.experimental.pallas import tpu as pltpu
from jax.sharding import PartitionSpec as P

MESH = pl.DeviceIdType.MESH
DEPTH = 4
WIDTH = 2048
CHUNK = 256
EXCHANGE_AT = 2
RELAY_AT = 13
SPLIT = (2, 4, 4, 2)
spectral_bound = 8.5
scale = 2.0 / spectral_bound


def rolled(v, shift):
    return pltpu.roll(v, shift % v.shape[1], 1)


def lookup(codes, table, count, factor):
    result = jnp.zeros(codes.shape, jnp.float32)
    for k in range(count):
        result = jnp.where(codes == k, table[k] * factor, result)
    return result


def kernel(
    dims,
    signs,
    disorder,
    bonds,
    onsite_table,
    hop_table,
    out,
    codes,
    fields,
    bonds_y,
    raw,
    relay_buf,
    relay_codes,
    base,
    right_1,
    right_2,
    right_3,
    left_0,
    left_1,
    left_2,
    left_3,
    drift_1,
    drift_2,
    drift_3,
    acc,
    packed,
    core_in,
    plane_buf,
    z_buf,
    final,
    row_sem,
    code_sem,
    row_send,
    row_recv,
    code_send,
    code_recv,
    relay_sem,
    red_send,
    red_recv,
):
    n_hi, n_x, n_y, n_core, n_lo = dims
    n_site = n_hi * n_x * n_y * n_core
    n_z = n_hi * n_lo
    rows = signs.shape[1]
    total = rows + 2 * DEPTH
    cols = signs.shape[2]
    site = lax.axis_index("site")
    vec = lax.axis_index("vec")
    core = lax.rem(site, n_core)
    y = lax.rem(site // n_core, n_y)
    x = lax.rem(site // (n_core * n_y), n_x)
    z = (site // (n_core * n_y * n_x)) * n_lo + vec

    def device(xx, yy, zz, cc):
        return (
            (zz // n_lo) * (n_x * n_y * n_core) + xx * (n_y * n_core) + yy * n_core + cc,
            lax.rem(zz, n_lo),
        )

    def is_last(xx, yy):
        return (xx // (n_x - 1)) * (yy // (n_y - 1))

    def around(k):
        return lax.rem(z + k + n_z, n_z)

    partner = (site + 1 - 2 * core, vec)
    across = (lax.rem(site + n_site + 2 * core - 1, n_site), vec)
    summing = core == 1 - is_last(x, y)
    plane_peers = []
    for j in range(n_x):
        for k in range(n_y):
            if j or k:
                xx, yy = lax.rem(x + j, n_x), lax.rem(y + k, n_y)
                plane_peers.append(device(xx, yy, z, 1 - is_last(xx, yy)))
    z_peers = [device(x, y, around(k), core) for k in range(1, n_z)]

    def count(flag):
        return flag.astype(jnp.int32)

    mirror_x = core * x + (1 - core) * (n_x - 1 - x)
    mirror_y = core * y + (1 - core) * (n_y - 1 - y)
    crossing = jnp.logical_and(mirror_x == n_x - 1, mirror_y == n_y - 1)
    by_end = jnp.logical_and(mirror_x == 0, mirror_y == n_y - 1)
    by_next = jnp.logical_and(mirror_x == n_x - 2, mirror_y == n_y - 1)
    by_z = jnp.logical_and(mirror_x == 0, mirror_y == 0)
    by_x = jnp.logical_or(by_end, by_next)
    relaying = jnp.logical_or(by_x, by_z)
    plane = n_x * n_y * n_core
    half = n_z // 2
    far_x, far_y = core * (n_x - 1), core * (n_y - 1)
    near_x, near_y = (1 - core) * (n_x - 1), (1 - core) * (n_y - 1)
    next_x = core * (n_x - 2) + (1 - core)
    source_core = core + count(by_z) * (1 - 2 * core)

    def relay_of(i):
        if i == 0:
            return device(near_x, far_y, z, core)
        if i == 2:
            return device(next_x, far_y, z, core)
        return device(far_x, far_y, around(i - 2), 1 - core)

    def relay_to(k):
        zz = around(half + count(by_z)) if k == 0 else around(half - 1)
        return ((zz // n_lo) * plane + (1 - source_core) * (plane - 1), lax.rem(zz, n_lo))

    barrier = pltpu.get_barrier_semaphore()

    def greet(peers):
        for peer in peers:
            pl.semaphore_signal(barrier, inc=1, device_id=peer, device_id_type=MESH)

    @pl.when(by_x)
    def _():
        greet([device(far_x, far_y, z, core)])

    @pl.when(by_z)
    def _():
        greet([device(x, y, around(k), 1 - core) for k in (1, -1)])

    @pl.when(crossing)
    def _():
        other_next = (1 - core) * (n_x - 2) + core
        greet(
            [
                device(far_x, near_y, around(half), 1 - core),
                device(other_next, near_y, around(half), 1 - core),
                device(near_x, near_y, around(half - 1), core),
                device(near_x, near_y, around(half + 1), core),
            ]
        )

    greet([partner])

    @pl.when(jnp.logical_not(crossing))
    def _():
        greet([across])

    @pl.when(summing)
    def _():
        greet(plane_peers + z_peers)

    n_greeted = (
        2 + count(summing) * (len(plane_peers) + len(z_peers)) + 3 * count(crossing) + count(by_x) + 2 * count(by_z)
    )

    def mine(k):
        return pltpu.make_async_copy(signs.at[:, k], raw.at[DEPTH + k], row_sem.at[k])

    def far_row(i):
        return core * (rows - 1 - i) + (1 - core) * i

    def near_row(i):
        return (1 - core) * (rows - 1 - i) + core * i

    for i in range(DEPTH):
        mine(far_row(i)).start()
    own_codes = [
        pltpu.make_async_copy(src, codes.at[j, pl.ds(0, rows)], code_sem.at[j])
        for j, src in enumerate((disorder, bonds.at[0], bonds.at[1]))
    ]
    for copy in own_codes:
        copy.start()
    for i in range(DEPTH):
        mine(near_row(i)).start()
    for i in range(DEPTH, rows - DEPTH):
        mine(i).start()

    def place(n):
        return lax.rem(n + total - DEPTH, total)

    def landing(side, i, source=None):
        flag = core if side == 0 else 1 - (core if source is None else source)
        return flag * (DEPTH + rows + i) + (1 - flag) * (DEPTH - 1 - i)

    def send_row(side, i, by_relay=False):
        own = near_row(i) if side == 0 else far_row(i)
        return pltpu.make_async_remote_copy(
            src_ref=raw.at[DEPTH + own],
            dst_ref=relay_buf.at[i // 3] if by_relay else raw.at[landing(side, i)],
            send_sem=row_send.at[side, i],
            recv_sem=relay_sem.at[0, i // 3] if by_relay else row_recv.at[side, i],
            device_id=relay_of(i) if by_relay else (partner if side == 0 else across),
            device_id_type=MESH,
        )

    def send_far_codes(i, by_relay=False):
        return pltpu.make_async_remote_copy(
            src_ref=codes.at[:, far_row(i)],
            dst_ref=relay_codes.at[:, i // 3] if by_relay else codes.at[:, place(landing(1, i))],
            send_sem=code_send.at[1, i],
            recv_sem=relay_sem.at[1, i // 3] if by_relay else code_recv.at[1, i],
            device_id=relay_of(i) if by_relay else across,
            device_id_type=MESH,
        )

    def relays(k):
        i = count(by_z) + 2 * count(by_next) if k == 0 else 3
        n = landing(1, i, source_core)
        return [
            pltpu.make_async_remote_copy(
                src_ref=src, dst_ref=dst, send_sem=relay_sem.at[2 + j, k], recv_sem=sem.at[1, i], device_id=relay_to(k), device_id_type=MESH
            )
            for j, (src, dst, sem) in enumerate(
                ((relay_buf.at[k], raw.at[n], row_recv), (relay_codes.at[:, k], codes.at[:, place(n)], code_recv))
            )
        ]

    def relay_on(k):
        row, code = relays(k)
        pltpu.make_async_copy(codes.at[:, 0], relay_codes.at[:, k], relay_sem.at[1, k]).wait()
        code.start()
        pltpu.make_async_copy(signs.at[:, 0], relay_buf.at[k], relay_sem.at[0, k]).wait()
        row.start()

    def send_codes(upward, j):
        src = rows - DEPTH if upward else 0
        dst = rows + DEPTH if upward else rows
        return pltpu.make_async_remote_copy(
            src_ref=codes.at[j, pl.ds(src, DEPTH)],
            dst_ref=codes.at[j, pl.ds(dst, DEPTH)],
            send_sem=code_send.at[0, j],
            recv_sem=code_recv.at[0, j],
            device_id=partner,
            device_id_type=MESH,
        )

    def exchange():
        pl.semaphore_wait(barrier, n_greeted)
        for i in range(DEPTH):

            @pl.when(crossing)
            def _(i=i):
                send_row(1, i, True).start()
                send_far_codes(i, True).start()

            @pl.when(jnp.logical_not(crossing))
            def _(i=i):
                send_row(1, i).start()
                send_far_codes(i).start()

        @pl.when(core == 1)
        def _():
            for j in range(3):
                send_codes(False, j).start()

        @pl.when(core == 0)
        def _():
            for j in range(3):
                send_codes(True, j).start()

        for i in range(DEPTH):
            send_row(0, i).start()

    def decode(start, size, first):
        at = pl.ds(start, size)
        onsite = lookup(codes[0, at, :], onsite_table, onsite_table.shape[0], scale)
        hop_x = lookup(codes[1, at, :], hop_table, hop_table.shape[0], -scale)
        hop_y = lookup(codes[2, at, :], hop_table, hop_table.shape[0], -scale)
        hop_back = rolled(hop_x, 1)
        for i in range(size):
            n = first + i
            s = core * n + (1 - core) * (total - 1 - n)
            for j, value in enumerate((onsite, hop_x, hop_back)):
                fields[j, s] = jnp.broadcast_to(value[i : i + 1], (8, cols))
            bonds_y[core * (n + 1) + (1 - core) * (total - 1 - n)] = jnp.broadcast_to(hop_y[i : i + 1], (8, cols))

    def decode_side(side):
        upper = side == 1
        if side == 0:
            for j in range(3):
                send_codes(True, j).wait_recv()
        else:
            for i in range(DEPTH):
                send_far_codes(i).wait_recv()

        @pl.when(core == 1)
        def _():
            decode(rows if upper else rows + DEPTH, DEPTH, rows + DEPTH if upper else 0)

        @pl.when(core == 0)
        def _():
            decode(rows + DEPTH if upper else rows, DEPTH, 0 if upper else rows + DEPTH)

    for copy in own_codes:
        copy.wait()
    for start in range(0, rows, 8):
        decode(start, 8, DEPTH + start)
    for i in range(rows):
        mine(i).wait()

    def natural(s):
        return core * s + (1 - core) * (total - 1 - s)

    def split(v):
        high = v.astype(jnp.bfloat16).astype(jnp.float32)
        return jnp.concatenate([high, v - high], axis=0).astype(jnp.bfloat16)

    def advance(t, levels, step=1):
        for lo in range(0, cols, WIDTH):
            here = pl.ds(lo, WIDTH)
            right = pl.ds((lo + WIDTH) % cols, 128)
            left = pl.ds((lo - 128) % cols, 128)

            def wide(v):
                return jnp.concatenate([v, v], axis=0)

            def bond(s):
                return wide(bonds_y[s + 1, :, here])

            def columns(ref, v, s):
                ext = jnp.concatenate([ref[s, :, left], v, ref[s, :, right]], axis=1)
                following = rolled(ext, -1)[:, 128 : 128 + WIDTH]
                previous = rolled(ext, 1)[:, 128 : 128 + WIDTH]
                return wide(fields[0, s, :, here]) * v + wide(fields[1, s, :, here]) * following + wide(fields[2, s, :, here]) * previous

            def toward(s):
                return (bond(s), bond(s - 1)) if step == 1 else (bond(s - 1), bond(s))

            def minus(u, v):
                return u - v if step == 1 else v - u

            ahead = jnp.where(raw[natural(t), :, here] == 1, 1.0, -1.0).astype(jnp.float32)
            base[t, :, here] = ahead
            if levels >= 1:
                s = t - step
                up, down = toward(s)
                forth, back = up * ahead, down * base[s - step, :, here]
                left_new = minus(forth, back)
                left_0[s, :, here] = left_new
                right_new = columns(base, base[s, :, here], s) + (forth + back)
                right_1[s, :, here] = right_new
            if levels >= 2:
                s = t - 2 * step
                up, down = toward(s)
                forth, back = up * right_new, down * right_1[s - step, :, here]
                drift_1[s, :, here] = minus(forth, back)
                twice = base[s, :, here]
                right_new = columns(right_1, right_1[s, :, here], s) + (forth + back) - (twice + twice)
                right_2[s, :, here] = right_new
                left_new = columns(left_0, left_0[s, :, here], s) + (up * left_new + down * left_0[s - step, :, here])
                left_1[s, :, here] = left_new
            if levels >= 3:
                s = t - 3 * step
                up, down = toward(s)
                forth, back = up * right_new, down * right_2[s - step, :, here]
                drift_2[s, :, here] = minus(forth, back)
                right_new = columns(right_2, right_2[s, :, here], s) + (forth + back) - right_1[s, :, here]
                right_3[s, :, here] = right_new
                twice = left_0[s, :, here]
                left_new = columns(left_1, left_1[s, :, here], s) + (up * left_new + down * left_1[s - step, :, here]) - (twice + twice)
                left_2[s, :, here] = left_new
            if levels >= 4:
                s = t - 4 * step
                up, down = toward(s)
                drift_3[s, :, here] = minus(up * right_new, down * right_3[s - step, :, here])
                left_new = columns(left_2, left_2[s, :, here], s) + (up * left_new + down * left_2[s - step, :, here]) - left_1[s, :, here]
                left_3[s, :, here] = left_new

    def multiply(s):
        product = None
        for lo in range(0, cols, CHUNK):
            here = pl.ds(lo, CHUNK)
            order_0 = split(left_0[s, :, here])
            lefts = jnp.concatenate([order_0] + [split(ref[s, :, here]) for ref in (left_1, left_2, left_3)], axis=0)
            drifts = jnp.concatenate([order_0] + [split(ref[s, :, here]) for ref in (drift_1, drift_2, drift_3)], axis=0)
            part = lax.dot_general(lefts, drifts, (((1,), (1,)), ((), ())), preferred_element_type=jnp.float32)
            product = part if product is None else product + part
        acc[...] += product

    for levels in range(4):

        def warm(t, carry, levels=levels):
            advance(t, levels)
            return carry

        lax.fori_loop(DEPTH + 2 * levels, DEPTH + 2 * levels + 2, warm, 0)
        if levels == 0:
            pl.when(crossing)(exchange)
        if levels == EXCHANGE_AT:
            pl.when(jnp.logical_not(crossing))(exchange)

    first = 3 * DEPTH

    def inner(t, carry):
        @pl.when(t == first + 1)
        def _():
            acc[...] = jnp.zeros_like(acc)

        @pl.when(jnp.logical_and(relaying, t == RELAY_AT))
        def _():
            relay_on(0)

        @pl.when(jnp.logical_and(by_z, t == RELAY_AT))
        def _():
            relay_on(1)

        multiply(t - DEPTH - 1)
        advance(t, 4)
        return carry

    lax.fori_loop(first, rows + DEPTH, inner, 0)

    decode_side(0)
    for i in range(DEPTH):
        send_row(0, i).wait_recv()

    def near(k, carry):
        t = DEPTH - 1 - k
        multiply(t + DEPTH + 1 + (rows - 1 - 2 * DEPTH) * (t // (DEPTH - 1)))
        advance(t, 4, -1)
        return carry

    lax.fori_loop(0, DEPTH, near, 0)

    decode_side(1)

    def far(t, carry):
        pltpu.make_async_copy(signs.at[:, 0], raw.at[0], row_recv.at[1, t - (rows + DEPTH)]).wait()
        multiply(t - DEPTH - 1 - (rows - 1 - DEPTH) * ((total - 1 - t) // (DEPTH - 1)))
        advance(t, 4)
        return carry

    lax.fori_loop(rows + DEPTH, total, far, 0)
    multiply(total - DEPTH - 1)

    whole = jnp.concatenate([acc[32 * b : 32 * b + 16, :] + acc[32 * b + 16 : 32 * b + 32, :] for b in range(4)], axis=0)
    whole = whole + rolled(whole, -16)
    lane = lax.broadcasted_iota(jnp.int32, (32, 128), 1)
    packed[...] = jnp.where((lane // 16) % 2 == 0, whole[:32], rolled(whole[32:], 16)).reshape(2, 16, 128)

    def send(src, dst, k, peer):
        return pltpu.make_async_remote_copy(
            src_ref=src, dst_ref=dst, send_sem=red_send.at[k], recv_sem=red_recv.at[k], device_id=peer, device_id_type=MESH
        )

    give = send(packed, core_in, 0, partner)
    take = send(final, final, 1, partner)

    @pl.when(summing)
    def _():
        give.wait_recv()
        halves = [packed[k] + core_in[k] for k in range(2)]
        waits = []
        start = 2
        places = (x * n_y + y, z)
        groups = (plane_peers, z_peers)
        for step in range(2):
            now = []
            for k in range(2):
                axis = (step + k) % 2
                buf = (plane_buf, z_buf)[axis].at[step]
                buf[places[axis]] = halves[k]
                for peer in groups[axis]:
                    now.append(send(buf.at[places[axis]], buf.at[places[axis]], start, peer))
                    now[-1].start()
                    start += 1
            for copy in now:
                copy.wait_recv()
            waits += now
            for k in range(2):
                axis = (step + k) % 2
                buf = (plane_buf, z_buf)[axis].at[step]
                value = buf[0]
                for j in range(1, len(groups[axis]) + 1):
                    value = value + buf[j]
                halves[k] = value
        for k in range(2):
            final[k] = halves[k]
        take.start()
        for copy in waits:
            copy.wait_send()

    @pl.when(jnp.logical_not(summing))
    def _():
        give.start()
        take.wait_recv()

    done = final[...].reshape(32, 128)
    per_site = -1.0 / (n_site * rows * cols * n_lo) / (scale * scale)
    for p in range(4):
        strip = done[(p % 2) * 16 : (p % 2) * 16 + 16]
        for q in range(4):
            block = rolled(strip, -(q * 32 + (p // 2) * 16))
            factor = per_site * (0.5 if p else 1.0) * (0.5 if q else 1.0)
            out[p, q] = block[:, :16] * factor

    @pl.when(summing)
    def _():
        take.wait_send()

    @pl.when(jnp.logical_not(summing))
    def _():
        give.wait_send()

    @pl.when(relaying)
    def _():
        for copy in relays(0):
            copy.wait_send()

    @pl.when(by_z)
    def _():
        for copy in relays(1):
            copy.wait_send()

    for side in range(2):
        for i in range(DEPTH):
            send_row(side, i).wait_send()
    for j in range(3):
        send_codes(True, j).wait_send()
    for i in range(DEPTH):
        send_far_codes(i).wait_send()


def solution(mesh):
    n_hi, n_x, n_y, n_core = SPLIT
    n_lo = mesh.shape["vec"]
    dims = (mesh.shape["site"] // (n_x * n_y * n_core), n_x, n_y, n_core, n_lo)

    def shards(vector_signs, disorder, bond_types, onsite_table, hop_table):
        width, rows, cols = vector_signs.shape
        total = rows + 2 * DEPTH
        n_z = dims[0] * n_lo
        n_red = 2 + 2 * (n_x * n_y - 1) + 2 * (n_z - 1)
        full = pltpu.VMEM((total, width, cols), jnp.float32)
        anywhere = pl.BlockSpec(memory_space=pl.ANY)
        scalars = pl.BlockSpec(memory_space=pltpu.SMEM)
        return pl.pallas_call(
            functools.partial(kernel, dims),
            out_shape=jax.ShapeDtypeStruct((4, 4, width, width), jnp.float32),
            in_specs=[anywhere, anywhere, anywhere, scalars, scalars],
            out_specs=pl.BlockSpec(memory_space=pltpu.VMEM),
            scratch_shapes=[
                pltpu.VMEM((3, total, cols), jnp.int32),
                pltpu.VMEM((3, total, 8, cols), jnp.float32),
                pltpu.VMEM((total + 1, 8, cols), jnp.float32),
                pltpu.VMEM((total, width, cols), jnp.int32),
                pltpu.VMEM((2, width, cols), jnp.int32),
                pltpu.VMEM((3, 2, cols), jnp.int32),
                full,
                full,
                full,
                full,
                full,
                full,
                full,
                full,
                full,
                full,
                full,
                pltpu.VMEM((128, 128), jnp.float32),
                pltpu.VMEM((2, 16, 128), jnp.float32),
                pltpu.VMEM((2, 16, 128), jnp.float32),
                pltpu.VMEM((2, n_x * n_y, 16, 128), jnp.float32),
                pltpu.VMEM((2, n_z, 16, 128), jnp.float32),
                pltpu.VMEM((2, 16, 128), jnp.float32),
                pltpu.SemaphoreType.DMA((rows,)),
                pltpu.SemaphoreType.DMA((3,)),
                pltpu.SemaphoreType.DMA((2, DEPTH)),
                pltpu.SemaphoreType.DMA((2, DEPTH)),
                pltpu.SemaphoreType.DMA((2, DEPTH)),
                pltpu.SemaphoreType.DMA((2, DEPTH)),
                pltpu.SemaphoreType.DMA((4, 2)),
                pltpu.SemaphoreType.DMA((n_red,)),
                pltpu.SemaphoreType.DMA((n_red,)),
            ],
            compiler_params=pltpu.CompilerParams(
                collective_id=0, has_side_effects=True, vmem_limit_bytes=60 * 1024 * 1024
            ),
        )(vector_signs, disorder, bond_types, onsite_table, hop_table)

    return jax.shard_map(
        shards,
        mesh=mesh,
        in_specs=(P("vec", "site", None), P("site", None), P(None, "site", None), P(), P()),
        out_specs=P(),
        check_vma=False,
    )
```

```python
import functools

import jax
import jax.numpy as jnp
from jax import lax
from jax.experimental import pallas as pl
from jax.experimental.pallas import tpu as pltpu
from jax.sharding import PartitionSpec as P

MESH = pl.DeviceIdType.MESH
DEPTH = 4
WIDTH = 2048
CHUNK = 256
EXCHANGE_AT = 3
RELAY_AT = 14
SPLIT = (2, 4, 4, 2)
spectral_bound = 8.5
scale = 2.0 / spectral_bound


def rolled(v, shift):
    return pltpu.roll(v, shift % v.shape[1], 1)


def lookup(codes, table, count, factor):
    result = jnp.zeros(codes.shape, jnp.float32)
    for k in range(count):
        result = jnp.where(codes == k, table[k] * factor, result)
    return result


def kernel(
    dims,
    signs,
    disorder,
    bonds,
    onsite_table,
    hop_table,
    out,
    codes,
    fields,
    bonds_y,
    raw,
    relay_buf,
    relay_codes,
    base,
    right_1,
    right_2,
    right_3,
    left_0,
    left_1,
    left_2,
    left_3,
    drift_1,
    drift_2,
    drift_3,
    acc,
    packed,
    core_in,
    plane_buf,
    z_buf,
    final,
    row_sem,
    code_sem,
    row_send,
    row_recv,
    code_send,
    code_recv,
    relay_sem,
    red_send,
    red_recv,
):
    n_hi, n_x, n_y, n_core, n_lo = dims
    n_site = n_hi * n_x * n_y * n_core
    n_z = n_hi * n_lo
    rows = signs.shape[1]
    total = rows + 2 * DEPTH
    cols = signs.shape[2]
    site = lax.axis_index("site")
    vec = lax.axis_index("vec")
    core = lax.rem(site, n_core)
    y = lax.rem(site // n_core, n_y)
    x = lax.rem(site // (n_core * n_y), n_x)
    z = (site // (n_core * n_y * n_x)) * n_lo + vec

    def device(xx, yy, zz, cc):
        return (
            (zz // n_lo) * (n_x * n_y * n_core) + xx * (n_y * n_core) + yy * n_core + cc,
            lax.rem(zz, n_lo),
        )

    def is_last(xx, yy):
        return (xx // (n_x - 1)) * (yy // (n_y - 1))

    def around(k):
        return lax.rem(z + k + n_z, n_z)

    partner = (site + 1 - 2 * core, vec)
    across = (lax.rem(site + n_site + 2 * core - 1, n_site), vec)
    summing = core == 1 - is_last(x, y)
    plane_peers = []
    for j in range(n_x):
        for k in range(n_y):
            if j or k:
                xx, yy = lax.rem(x + j, n_x), lax.rem(y + k, n_y)
                plane_peers.append(device(xx, yy, z, 1 - is_last(xx, yy)))
    z_peers = [device(x, y, around(k), core) for k in range(1, n_z)]

    def count(flag):
        return flag.astype(jnp.int32)

    mirror_x = core * x + (1 - core) * (n_x - 1 - x)
    mirror_y = core * y + (1 - core) * (n_y - 1 - y)
    crossing = jnp.logical_and(mirror_x == n_x - 1, mirror_y == n_y - 1)
    by_end = jnp.logical_and(mirror_x == 0, mirror_y == n_y - 1)
    by_next = jnp.logical_and(mirror_x == n_x - 2, mirror_y == n_y - 1)
    by_z = jnp.logical_and(mirror_x == 0, mirror_y == 0)
    by_x = jnp.logical_or(by_end, by_next)
    relaying = jnp.logical_or(by_x, by_z)
    plane = n_x * n_y * n_core
    half = n_z // 2
    far_x, far_y = core * (n_x - 1), core * (n_y - 1)
    near_x, near_y = (1 - core) * (n_x - 1), (1 - core) * (n_y - 1)
    next_x = core * (n_x - 2) + (1 - core)
    source_core = core + count(by_z) * (1 - 2 * core)

    def relay_of(i):
        if i == 0:
            return device(near_x, far_y, z, core)
        if i == 2:
            return device(next_x, far_y, z, core)
        return device(far_x, far_y, around(i - 2), 1 - core)

    def relay_to(k):
        zz = around(half + count(by_z)) if k == 0 else around(half - 1)
        return ((zz // n_lo) * plane + (1 - source_core) * (plane - 1), lax.rem(zz, n_lo))

    barrier = pltpu.get_barrier_semaphore()

    def greet(peers):
        for peer in peers:
            pl.semaphore_signal(barrier, inc=1, device_id=peer, device_id_type=MESH)

    @pl.when(by_x)
    def _():
        greet([device(far_x, far_y, z, core)])

    @pl.when(by_z)
    def _():
        greet([device(x, y, around(k), 1 - core) for k in (1, -1)])

    @pl.when(crossing)
    def _():
        other_next = (1 - core) * (n_x - 2) + core
        greet(
            [
                device(far_x, near_y, around(half), 1 - core),
                device(other_next, near_y, around(half), 1 - core),
                device(near_x, near_y, around(half - 1), core),
                device(near_x, near_y, around(half + 1), core),
            ]
        )

    greet([partner])

    @pl.when(jnp.logical_not(crossing))
    def _():
        greet([across])

    @pl.when(summing)
    def _():
        greet(plane_peers + z_peers)

    n_greeted = (
        2 + count(summing) * (len(plane_peers) + len(z_peers)) + 3 * count(crossing) + count(by_x) + 2 * count(by_z)
    )

    def mine(k):
        return pltpu.make_async_copy(signs.at[:, k], raw.at[DEPTH + k], row_sem.at[k])

    def far_row(i):
        return core * (rows - 1 - i) + (1 - core) * i

    def near_row(i):
        return (1 - core) * (rows - 1 - i) + core * i

    for i in range(DEPTH):
        mine(far_row(i)).start()
    own_codes = [
        pltpu.make_async_copy(src, codes.at[j, pl.ds(0, rows)], code_sem.at[j])
        for j, src in enumerate((disorder, bonds.at[0], bonds.at[1]))
    ]
    for copy in own_codes:
        copy.start()
    for i in range(DEPTH):
        mine(near_row(i)).start()
    for i in range(DEPTH, rows - DEPTH):
        mine(i).start()

    def place(n):
        return lax.rem(n + total - DEPTH, total)

    def landing(side, i, source=None):
        flag = core if side == 0 else 1 - (core if source is None else source)
        return flag * (DEPTH + rows + i) + (1 - flag) * (DEPTH - 1 - i)

    def send_row(side, i, by_relay=False):
        own = near_row(i) if side == 0 else far_row(i)
        return pltpu.make_async_remote_copy(
            src_ref=raw.at[DEPTH + own],
            dst_ref=relay_buf.at[i // 3] if by_relay else raw.at[landing(side, i)],
            send_sem=row_send.at[side, i],
            recv_sem=relay_sem.at[0, i // 3] if by_relay else row_recv.at[side, i],
            device_id=relay_of(i) if by_relay else (partner if side == 0 else across),
            device_id_type=MESH,
        )

    def send_far_codes(i, by_relay=False):
        return pltpu.make_async_remote_copy(
            src_ref=codes.at[:, far_row(i)],
            dst_ref=relay_codes.at[:, i // 3] if by_relay else codes.at[:, place(landing(1, i))],
            send_sem=code_send.at[1, i],
            recv_sem=relay_sem.at[1, i // 3] if by_relay else code_recv.at[1, i],
            device_id=relay_of(i) if by_relay else across,
            device_id_type=MESH,
        )

    def relays(k):
        i = count(by_z) + 2 * count(by_next) if k == 0 else 3
        n = landing(1, i, source_core)
        return [
            pltpu.make_async_remote_copy(
                src_ref=src, dst_ref=dst, send_sem=relay_sem.at[2 + j, k], recv_sem=sem.at[1, i], device_id=relay_to(k), device_id_type=MESH
            )
            for j, (src, dst, sem) in enumerate(
                ((relay_buf.at[k], raw.at[n], row_recv), (relay_codes.at[:, k], codes.at[:, place(n)], code_recv))
            )
        ]

    def relay_on(k):
        row, code = relays(k)
        pltpu.make_async_copy(codes.at[:, 0], relay_codes.at[:, k], relay_sem.at[1, k]).wait()
        code.start()
        pltpu.make_async_copy(signs.at[:, 0], relay_buf.at[k], relay_sem.at[0, k]).wait()
        row.start()

    def send_codes(upward, j):
        src = rows - DEPTH if upward else 0
        dst = rows + DEPTH if upward else rows
        return pltpu.make_async_remote_copy(
            src_ref=codes.at[j, pl.ds(src, DEPTH)],
            dst_ref=codes.at[j, pl.ds(dst, DEPTH)],
            send_sem=code_send.at[0, j],
            recv_sem=code_recv.at[0, j],
            device_id=partner,
            device_id_type=MESH,
        )

    def exchange():
        pl.semaphore_wait(barrier, n_greeted)
        for i in range(DEPTH):

            @pl.when(crossing)
            def _(i=i):
                send_row(1, i, True).start()
                send_far_codes(i, True).start()

            @pl.when(jnp.logical_not(crossing))
            def _(i=i):
                send_row(1, i).start()
                send_far_codes(i).start()

        @pl.when(core == 1)
        def _():
            for j in range(3):
                send_codes(False, j).start()

        @pl.when(core == 0)
        def _():
            for j in range(3):
                send_codes(True, j).start()

        for i in range(DEPTH):
            send_row(0, i).start()

    def decode(start, size, first):
        at = pl.ds(start, size)
        onsite = lookup(codes[0, at, :], onsite_table, onsite_table.shape[0], scale)
        hop_x = lookup(codes[1, at, :], hop_table, hop_table.shape[0], -scale)
        hop_y = lookup(codes[2, at, :], hop_table, hop_table.shape[0], -scale)
        hop_back = rolled(hop_x, 1)
        for i in range(size):
            n = first + i
            s = core * n + (1 - core) * (total - 1 - n)
            for j, value in enumerate((onsite, hop_x, hop_back)):
                fields[j, s] = jnp.broadcast_to(value[i : i + 1], (8, cols))
            bonds_y[core * (n + 1) + (1 - core) * (total - 1 - n)] = jnp.broadcast_to(hop_y[i : i + 1], (8, cols))

    def decode_side(side):
        upper = side == 1
        if side == 0:
            for j in range(3):
                send_codes(True, j).wait_recv()
        else:
            for i in range(DEPTH):
                send_far_codes(i).wait_recv()

        @pl.when(core == 1)
        def _():
            decode(rows if upper else rows + DEPTH, DEPTH, rows + DEPTH if upper else 0)

        @pl.when(core == 0)
        def _():
            decode(rows + DEPTH if upper else rows, DEPTH, 0 if upper else rows + DEPTH)

    for copy in own_codes:
        copy.wait()
    for start in range(0, rows, 8):
        decode(start, 8, DEPTH + start)
    for i in range(rows):
        mine(i).wait()

    def natural(s):
        return core * s + (1 - core) * (total - 1 - s)

    def split(v):
        high = v.astype(jnp.bfloat16).astype(jnp.float32)
        return jnp.concatenate([high, v - high], axis=0).astype(jnp.bfloat16)

    def advance(t, levels, step=1):
        for lo in range(0, cols, WIDTH):
            here = pl.ds(lo, WIDTH)
            right = pl.ds((lo + WIDTH) % cols, 128)
            left = pl.ds((lo - 128) % cols, 128)

            def wide(v):
                return jnp.concatenate([v, v], axis=0)

            def bond(s):
                return wide(bonds_y[s + 1, :, here])

            def columns(ref, v, s):
                ext = jnp.concatenate([ref[s, :, left], v, ref[s, :, right]], axis=1)
                following = rolled(ext, -1)[:, 128 : 128 + WIDTH]
                previous = rolled(ext, 1)[:, 128 : 128 + WIDTH]
                return wide(fields[0, s, :, here]) * v + wide(fields[1, s, :, here]) * following + wide(fields[2, s, :, here]) * previous

            def toward(s):
                return (bond(s), bond(s - 1)) if step == 1 else (bond(s - 1), bond(s))

            def minus(u, v):
                return u - v if step == 1 else v - u

            ahead = jnp.where(raw[natural(t), :, here] == 1, 1.0, -1.0).astype(jnp.float32)
            base[t, :, here] = ahead
            if levels >= 1:
                s = t - step
                up, down = toward(s)
                forth, back = up * ahead, down * base[s - step, :, here]
                left_new = minus(forth, back)
                left_0[s, :, here] = left_new
                right_new = columns(base, base[s, :, here], s) + (forth + back)
                right_1[s, :, here] = right_new
            if levels >= 2:
                s = t - 2 * step
                up, down = toward(s)
                forth, back = up * right_new, down * right_1[s - step, :, here]
                drift_1[s, :, here] = minus(forth, back)
                twice = base[s, :, here]
                right_new = columns(right_1, right_1[s, :, here], s) + (forth + back) - (twice + twice)
                right_2[s, :, here] = right_new
                left_new = columns(left_0, left_0[s, :, here], s) + (up * left_new + down * left_0[s - step, :, here])
                left_1[s, :, here] = left_new
            if levels >= 3:
                s = t - 3 * step
                up, down = toward(s)
                forth, back = up * right_new, down * right_2[s - step, :, here]
                drift_2[s, :, here] = minus(forth, back)
                right_new = columns(right_2, right_2[s, :, here], s) + (forth + back) - right_1[s, :, here]
                right_3[s, :, here] = right_new
                twice = left_0[s, :, here]
                left_new = columns(left_1, left_1[s, :, here], s) + (up * left_new + down * left_1[s - step, :, here]) - (twice + twice)
                left_2[s, :, here] = left_new
            if levels >= 4:
                s = t - 4 * step
                up, down = toward(s)
                drift_3[s, :, here] = minus(up * right_new, down * right_3[s - step, :, here])
                left_new = columns(left_2, left_2[s, :, here], s) + (up * left_new + down * left_2[s - step, :, here]) - left_1[s, :, here]
                left_3[s, :, here] = left_new

    def multiply(s):
        product = None
        for lo in range(0, cols, CHUNK):
            here = pl.ds(lo, CHUNK)
            order_0 = split(left_0[s, :, here])
            lefts = jnp.concatenate([order_0] + [split(ref[s, :, here]) for ref in (left_1, left_2, left_3)], axis=0)
            drifts = jnp.concatenate([order_0] + [split(ref[s, :, here]) for ref in (drift_1, drift_2, drift_3)], axis=0)
            part = lax.dot_general(lefts, drifts, (((1,), (1,)), ((), ())), preferred_element_type=jnp.float32)
            product = part if product is None else product + part
        acc[...] += product

    for levels in range(4):

        def warm(t, carry, levels=levels):
            advance(t, levels)
            return carry

        lax.fori_loop(DEPTH + 2 * levels, DEPTH + 2 * levels + 2, warm, 0)
        if levels == 0:
            pl.when(crossing)(exchange)
        if levels == EXCHANGE_AT:
            pl.when(jnp.logical_not(crossing))(exchange)

    first = 3 * DEPTH

    def inner(t, carry):
        @pl.when(t == first + 1)
        def _():
            acc[...] = jnp.zeros_like(acc)

        @pl.when(jnp.logical_and(relaying, t == RELAY_AT))
        def _():
            relay_on(0)

        @pl.when(jnp.logical_and(by_z, t == RELAY_AT))
        def _():
            relay_on(1)

        multiply(t - DEPTH - 1)
        advance(t, 4)
        return carry

    lax.fori_loop(first, rows + DEPTH, inner, 0)

    decode_side(0)
    for i in range(DEPTH):
        send_row(0, i).wait_recv()

    def near(k, carry):
        t = DEPTH - 1 - k
        multiply(t + DEPTH + 1 + (rows - 1 - 2 * DEPTH) * (t // (DEPTH - 1)))
        advance(t, 4, -1)
        return carry

    lax.fori_loop(0, DEPTH, near, 0)

    decode_side(1)

    def far(t, carry):
        pltpu.make_async_copy(signs.at[:, 0], raw.at[0], row_recv.at[1, t - (rows + DEPTH)]).wait()
        multiply(t - DEPTH - 1 - (rows - 1 - DEPTH) * ((total - 1 - t) // (DEPTH - 1)))
        advance(t, 4)
        return carry

    lax.fori_loop(rows + DEPTH, total, far, 0)
    multiply(total - DEPTH - 1)

    whole = jnp.concatenate([acc[32 * b : 32 * b + 16, :] + acc[32 * b + 16 : 32 * b + 32, :] for b in range(4)], axis=0)
    whole = whole + rolled(whole, -16)
    lane = lax.broadcasted_iota(jnp.int32, (32, 128), 1)
    packed[...] = jnp.where((lane // 16) % 2 == 0, whole[:32], rolled(whole[32:], 16)).reshape(2, 16, 128)

    def send(src, dst, k, peer):
        return pltpu.make_async_remote_copy(
            src_ref=src, dst_ref=dst, send_sem=red_send.at[k], recv_sem=red_recv.at[k], device_id=peer, device_id_type=MESH
        )

    give = send(packed, core_in, 0, partner)
    take = send(final, final, 1, partner)

    @pl.when(summing)
    def _():
        give.wait_recv()
        halves = [packed[k] + core_in[k] for k in range(2)]
        waits = []
        start = 2
        places = (x * n_y + y, z)
        groups = (plane_peers, z_peers)
        for step in range(2):
            now = []
            for k in range(2):
                axis = (step + k) % 2
                buf = (plane_buf, z_buf)[axis].at[step]
                buf[places[axis]] = halves[k]
                for peer in groups[axis]:
                    now.append(send(buf.at[places[axis]], buf.at[places[axis]], start, peer))
                    now[-1].start()
                    start += 1
            for copy in now:
                copy.wait_recv()
            waits += now
            for k in range(2):
                axis = (step + k) % 2
                buf = (plane_buf, z_buf)[axis].at[step]
                value = buf[0]
                for j in range(1, len(groups[axis]) + 1):
                    value = value + buf[j]
                halves[k] = value
        for k in range(2):
            final[k] = halves[k]
        take.start()
        for copy in waits:
            copy.wait_send()

    @pl.when(jnp.logical_not(summing))
    def _():
        give.start()
        take.wait_recv()

    done = final[...].reshape(32, 128)
    per_site = -1.0 / (n_site * rows * cols * n_lo) / (scale * scale)
    for p in range(4):
        strip = done[(p % 2) * 16 : (p % 2) * 16 + 16]
        for q in range(4):
            block = rolled(strip, -(q * 32 + (p // 2) * 16))
            factor = per_site * (0.5 if p else 1.0) * (0.5 if q else 1.0)
            out[p, q] = block[:, :16] * factor

    @pl.when(summing)
    def _():
        take.wait_send()

    @pl.when(jnp.logical_not(summing))
    def _():
        give.wait_send()

    @pl.when(relaying)
    def _():
        for copy in relays(0):
            copy.wait_send()

    @pl.when(by_z)
    def _():
        for copy in relays(1):
            copy.wait_send()

    for side in range(2):
        for i in range(DEPTH):
            send_row(side, i).wait_send()
    for j in range(3):
        send_codes(True, j).wait_send()
    for i in range(DEPTH):
        send_far_codes(i).wait_send()


def solution(mesh):
    n_hi, n_x, n_y, n_core = SPLIT
    n_lo = mesh.shape["vec"]
    dims = (mesh.shape["site"] // (n_x * n_y * n_core), n_x, n_y, n_core, n_lo)

    def shards(vector_signs, disorder, bond_types, onsite_table, hop_table):
        width, rows, cols = vector_signs.shape
        total = rows + 2 * DEPTH
        n_z = dims[0] * n_lo
        n_red = 2 + 2 * (n_x * n_y - 1) + 2 * (n_z - 1)
        full = pltpu.VMEM((total, width, cols), jnp.float32)
        anywhere = pl.BlockSpec(memory_space=pl.ANY)
        scalars = pl.BlockSpec(memory_space=pltpu.SMEM)
        return pl.pallas_call(
            functools.partial(kernel, dims),
            out_shape=jax.ShapeDtypeStruct((4, 4, width, width), jnp.float32),
            in_specs=[anywhere, anywhere, anywhere, scalars, scalars],
            out_specs=pl.BlockSpec(memory_space=pltpu.VMEM),
            scratch_shapes=[
                pltpu.VMEM((3, total, cols), jnp.int32),
                pltpu.VMEM((3, total, 8, cols), jnp.float32),
                pltpu.VMEM((total + 1, 8, cols), jnp.float32),
                pltpu.VMEM((total, width, cols), jnp.int32),
                pltpu.VMEM((2, width, cols), jnp.int32),
                pltpu.VMEM((3, 2, cols), jnp.int32),
                full,
                full,
                full,
                full,
                full,
                full,
                full,
                full,
                full,
                full,
                full,
                pltpu.VMEM((128, 128), jnp.float32),
                pltpu.VMEM((2, 16, 128), jnp.float32),
                pltpu.VMEM((2, 16, 128), jnp.float32),
                pltpu.VMEM((2, n_x * n_y, 16, 128), jnp.float32),
                pltpu.VMEM((2, n_z, 16, 128), jnp.float32),
                pltpu.VMEM((2, 16, 128), jnp.float32),
                pltpu.SemaphoreType.DMA((rows,)),
                pltpu.SemaphoreType.DMA((3,)),
                pltpu.SemaphoreType.DMA((2, DEPTH)),
                pltpu.SemaphoreType.DMA((2, DEPTH)),
                pltpu.SemaphoreType.DMA((2, DEPTH)),
                pltpu.SemaphoreType.DMA((2, DEPTH)),
                pltpu.SemaphoreType.DMA((4, 2)),
                pltpu.SemaphoreType.DMA((n_red,)),
                pltpu.SemaphoreType.DMA((n_red,)),
            ],
            compiler_params=pltpu.CompilerParams(
                collective_id=0, has_side_effects=True, vmem_limit_bytes=60 * 1024 * 1024
            ),
        )(vector_signs, disorder, bond_types, onsite_table, hop_table)

    return jax.shard_map(
        shards,
        mesh=mesh,
        in_specs=(P("vec", "site", None), P("site", None), P(None, "site", None), P(), P()),
        out_specs=P(),
        check_vma=False,
    )
```

```python
import functools

import jax
import jax.numpy as jnp
from jax import lax
from jax.experimental import pallas as pl
from jax.experimental.pallas import tpu as pltpu
from jax.sharding import PartitionSpec as P

MESH = pl.DeviceIdType.MESH
DEPTH = 4
WIDTH = 2048
CHUNK = 256
EXCHANGE_AT = 1
RELAY_AT = 14
SPLIT = (2, 4, 4, 2)
spectral_bound = 8.5
scale = 2.0 / spectral_bound


def rolled(v, shift):
    return pltpu.roll(v, shift % v.shape[1], 1)


def lookup(codes, table, count, factor):
    result = jnp.zeros(codes.shape, jnp.float32)
    for k in range(count):
        result = jnp.where(codes == k, table[k] * factor, result)
    return result


def kernel(
    dims,
    signs,
    disorder,
    bonds,
    onsite_table,
    hop_table,
    out,
    codes,
    fields,
    bonds_y,
    raw,
    relay_buf,
    relay_codes,
    base,
    right_1,
    right_2,
    right_3,
    left_0,
    left_1,
    left_2,
    left_3,
    drift_1,
    drift_2,
    drift_3,
    acc,
    packed,
    core_in,
    plane_buf,
    z_buf,
    final,
    row_sem,
    code_sem,
    row_send,
    row_recv,
    code_send,
    code_recv,
    relay_sem,
    round_sem,
    red_send,
    red_recv,
):
    n_hi, n_x, n_y, n_core, n_lo = dims
    n_site = n_hi * n_x * n_y * n_core
    n_z = n_hi * n_lo
    rows = signs.shape[1]
    total = rows + 2 * DEPTH
    cols = signs.shape[2]
    site = lax.axis_index("site")
    vec = lax.axis_index("vec")
    core = lax.rem(site, n_core)
    y = lax.rem(site // n_core, n_y)
    x = lax.rem(site // (n_core * n_y), n_x)
    z = (site // (n_core * n_y * n_x)) * n_lo + vec

    def device(xx, yy, zz, cc):
        return (
            (zz // n_lo) * (n_x * n_y * n_core) + xx * (n_y * n_core) + yy * n_core + cc,
            lax.rem(zz, n_lo),
        )

    def is_last(xx, yy):
        return (xx // (n_x - 1)) * (yy // (n_y - 1))

    def around(k):
        return lax.rem(z + k + n_z, n_z)

    partner = (site + 1 - 2 * core, vec)
    across = (lax.rem(site + n_site + 2 * core - 1, n_site), vec)
    summing = core == 1 - is_last(x, y)
    plane_peers = []
    for j in range(n_x):
        for k in range(n_y):
            if j or k:
                xx, yy = lax.rem(x + j, n_x), lax.rem(y + k, n_y)
                plane_peers.append(device(xx, yy, z, 1 - is_last(xx, yy)))
    z_peers = [device(x, y, around(k), core) for k in range(1, n_z)]

    next_chips = []
    for j, k in ((1, 0), (n_x - 1, 0), (0, 1), (0, n_y - 1)):
        xx, yy = lax.rem(x + j, n_x), lax.rem(y + k, n_y)
        next_chips.append(device(xx, yy, z, 1 - is_last(xx, yy)))
    next_chips += [device(x, y, around(k), core) for k in (1, -1)]

    def pass_on(heard, told):
        @pl.when(summing)
        def _():
            if heard is not None:
                pl.semaphore_wait(round_sem.at[heard], len(next_chips))
            if told is not None:
                for peer in next_chips:
                    pl.semaphore_signal(round_sem.at[told], inc=1, device_id=peer, device_id_type=MESH)

    def count(flag):
        return flag.astype(jnp.int32)

    mirror_x = core * x + (1 - core) * (n_x - 1 - x)
    mirror_y = core * y + (1 - core) * (n_y - 1 - y)
    crossing = jnp.logical_and(mirror_x == n_x - 1, mirror_y == n_y - 1)
    by_end = jnp.logical_and(mirror_x == 0, mirror_y == n_y - 1)
    by_next = jnp.logical_and(mirror_x == n_x - 2, mirror_y == n_y - 1)
    by_z = jnp.logical_and(mirror_x == 0, mirror_y == 0)
    by_x = jnp.logical_or(by_end, by_next)
    relaying = jnp.logical_or(by_x, by_z)
    plane = n_x * n_y * n_core
    half = n_z // 2
    far_x, far_y = core * (n_x - 1), core * (n_y - 1)
    near_x, near_y = (1 - core) * (n_x - 1), (1 - core) * (n_y - 1)
    next_x = core * (n_x - 2) + (1 - core)
    source_core = core + count(by_z) * (1 - 2 * core)

    def relay_of(i):
        if i == 0:
            return device(near_x, far_y, z, core)
        if i == 2:
            return device(next_x, far_y, z, core)
        return device(far_x, far_y, around(i - 2), 1 - core)

    def relay_to(k):
        zz = around(half + count(by_z)) if k == 0 else around(half - 1)
        return ((zz // n_lo) * plane + (1 - source_core) * (plane - 1), lax.rem(zz, n_lo))

    barrier = pltpu.get_barrier_semaphore()

    def greet(peers):
        for peer in peers:
            pl.semaphore_signal(barrier, inc=1, device_id=peer, device_id_type=MESH)

    @pl.when(by_x)
    def _():
        greet([device(far_x, far_y, z, core)])

    @pl.when(by_z)
    def _():
        greet([device(x, y, around(k), 1 - core) for k in (1, -1)])

    @pl.when(crossing)
    def _():
        other_next = (1 - core) * (n_x - 2) + core
        greet(
            [
                device(far_x, near_y, around(half), 1 - core),
                device(other_next, near_y, around(half), 1 - core),
                device(near_x, near_y, around(half - 1), core),
                device(near_x, near_y, around(half + 1), core),
            ]
        )

    greet([partner])

    @pl.when(jnp.logical_not(crossing))
    def _():
        greet([across])

    @pl.when(summing)
    def _():
        greet(next_chips)

    n_greeted = (
        2 + count(summing) * len(next_chips) + 3 * count(crossing) + count(by_x) + 2 * count(by_z)
    )

    def mine(k):
        return pltpu.make_async_copy(signs.at[:, k], raw.at[DEPTH + k], row_sem.at[k])

    def far_row(i):
        return core * (rows - 1 - i) + (1 - core) * i

    def near_row(i):
        return (1 - core) * (rows - 1 - i) + core * i

    for i in range(DEPTH):
        mine(far_row(i)).start()
    own_codes = [
        pltpu.make_async_copy(src, codes.at[j, pl.ds(0, rows)], code_sem.at[j])
        for j, src in enumerate((disorder, bonds.at[0], bonds.at[1]))
    ]
    for copy in own_codes:
        copy.start()
    for i in range(DEPTH):
        mine(near_row(i)).start()
    for i in range(DEPTH, rows - DEPTH):
        mine(i).start()

    def place(n):
        return lax.rem(n + total - DEPTH, total)

    def landing(side, i, source=None):
        flag = core if side == 0 else 1 - (core if source is None else source)
        return flag * (DEPTH + rows + i) + (1 - flag) * (DEPTH - 1 - i)

    def send_row(side, i, by_relay=False):
        own = near_row(i) if side == 0 else far_row(i)
        return pltpu.make_async_remote_copy(
            src_ref=raw.at[DEPTH + own],
            dst_ref=relay_buf.at[i // 3] if by_relay else raw.at[landing(side, i)],
            send_sem=row_send.at[side, i],
            recv_sem=relay_sem.at[0, i // 3] if by_relay else row_recv.at[side, i],
            device_id=relay_of(i) if by_relay else (partner if side == 0 else across),
            device_id_type=MESH,
        )

    def send_far_codes(i, by_relay=False):
        return pltpu.make_async_remote_copy(
            src_ref=codes.at[:, far_row(i)],
            dst_ref=relay_codes.at[:, i // 3] if by_relay else codes.at[:, place(landing(1, i))],
            send_sem=code_send.at[1, i],
            recv_sem=relay_sem.at[1, i // 3] if by_relay else code_recv.at[1, i],
            device_id=relay_of(i) if by_relay else across,
            device_id_type=MESH,
        )

    def relays(k):
        i = count(by_z) + 2 * count(by_next) if k == 0 else 3
        n = landing(1, i, source_core)
        return [
            pltpu.make_async_remote_copy(
                src_ref=src, dst_ref=dst, send_sem=relay_sem.at[2 + j, k], recv_sem=sem.at[1, i], device_id=relay_to(k), device_id_type=MESH
            )
            for j, (src, dst, sem) in enumerate(
                ((relay_buf.at[k], raw.at[n], row_recv), (relay_codes.at[:, k], codes.at[:, place(n)], code_recv))
            )
        ]

    def relay_on(k):
        row, code = relays(k)
        pltpu.make_async_copy(codes.at[:, 0], relay_codes.at[:, k], relay_sem.at[1, k]).wait()
        code.start()
        pltpu.make_async_copy(signs.at[:, 0], relay_buf.at[k], relay_sem.at[0, k]).wait()
        row.start()

    def send_codes(upward, j):
        src = rows - DEPTH if upward else 0
        dst = rows + DEPTH if upward else rows
        return pltpu.make_async_remote_copy(
            src_ref=codes.at[j, pl.ds(src, DEPTH)],
            dst_ref=codes.at[j, pl.ds(dst, DEPTH)],
            send_sem=code_send.at[0, j],
            recv_sem=code_recv.at[0, j],
            device_id=partner,
            device_id_type=MESH,
        )

    def exchange():
        pl.semaphore_wait(barrier, n_greeted)
        for i in range(DEPTH):

            @pl.when(crossing)
            def _(i=i):
                send_row(1, i, True).start()
                send_far_codes(i, True).start()

            @pl.when(jnp.logical_not(crossing))
            def _(i=i):
                send_row(1, i).start()
                send_far_codes(i).start()

        @pl.when(core == 1)
        def _():
            for j in range(3):
                send_codes(False, j).start()

        @pl.when(core == 0)
        def _():
            for j in range(3):
                send_codes(True, j).start()

        for i in range(DEPTH):
            send_row(0, i).start()

    def decode(start, size, first):
        at = pl.ds(start, size)
        onsite = lookup(codes[0, at, :], onsite_table, onsite_table.shape[0], scale)
        hop_x = lookup(codes[1, at, :], hop_table, hop_table.shape[0], -scale)
        hop_y = lookup(codes[2, at, :], hop_table, hop_table.shape[0], -scale)
        hop_back = rolled(hop_x, 1)
        for i in range(size):
            n = first + i
            s = core * n + (1 - core) * (total - 1 - n)
            for j, value in enumerate((onsite, hop_x, hop_back)):
                fields[j, s] = jnp.broadcast_to(value[i : i + 1], (8, cols))
            bonds_y[core * (n + 1) + (1 - core) * (total - 1 - n)] = jnp.broadcast_to(hop_y[i : i + 1], (8, cols))

    def decode_side(side):
        upper = side == 1
        if side == 0:
            for j in range(3):
                send_codes(True, j).wait_recv()
        else:
            for i in range(DEPTH):
                send_far_codes(i).wait_recv()

        @pl.when(core == 1)
        def _():
            decode(rows if upper else rows + DEPTH, DEPTH, rows + DEPTH if upper else 0)

        @pl.when(core == 0)
        def _():
            decode(rows + DEPTH if upper else rows, DEPTH, 0 if upper else rows + DEPTH)

    for copy in own_codes:
        copy.wait()
    for start in range(0, rows, 8):
        decode(start, 8, DEPTH + start)
    for i in range(rows):
        mine(i).wait()

    def natural(s):
        return core * s + (1 - core) * (total - 1 - s)

    def split(v):
        high = v.astype(jnp.bfloat16).astype(jnp.float32)
        return jnp.concatenate([high, v - high], axis=0).astype(jnp.bfloat16)

    def advance(t, levels, step=1):
        for lo in range(0, cols, WIDTH):
            here = pl.ds(lo, WIDTH)
            right = pl.ds((lo + WIDTH) % cols, 128)
            left = pl.ds((lo - 128) % cols, 128)

            def wide(v):
                return jnp.concatenate([v, v], axis=0)

            def bond(s):
                return wide(bonds_y[s + 1, :, here])

            def columns(ref, v, s):
                ext = jnp.concatenate([ref[s, :, left], v, ref[s, :, right]], axis=1)
                following = rolled(ext, -1)[:, 128 : 128 + WIDTH]
                previous = rolled(ext, 1)[:, 128 : 128 + WIDTH]
                return wide(fields[0, s, :, here]) * v + wide(fields[1, s, :, here]) * following + wide(fields[2, s, :, here]) * previous

            def toward(s):
                return (bond(s), bond(s - 1)) if step == 1 else (bond(s - 1), bond(s))

            def minus(u, v):
                return u - v if step == 1 else v - u

            ahead = jnp.where(raw[natural(t), :, here] == 1, 1.0, -1.0).astype(jnp.float32)
            base[t, :, here] = ahead
            if levels >= 1:
                s = t - step
                up, down = toward(s)
                forth, back = up * ahead, down * base[s - step, :, here]
                left_new = minus(forth, back)
                left_0[s, :, here] = left_new
                right_new = columns(base, base[s, :, here], s) + (forth + back)
                right_1[s, :, here] = right_new
            if levels >= 2:
                s = t - 2 * step
                up, down = toward(s)
                forth, back = up * right_new, down * right_1[s - step, :, here]
                drift_1[s, :, here] = minus(forth, back)
                twice = base[s, :, here]
                right_new = columns(right_1, right_1[s, :, here], s) + (forth + back) - (twice + twice)
                right_2[s, :, here] = right_new
                left_new = columns(left_0, left_0[s, :, here], s) + (up * left_new + down * left_0[s - step, :, here])
                left_1[s, :, here] = left_new
            if levels >= 3:
                s = t - 3 * step
                up, down = toward(s)
                forth, back = up * right_new, down * right_2[s - step, :, here]
                drift_2[s, :, here] = minus(forth, back)
                right_new = columns(right_2, right_2[s, :, here], s) + (forth + back) - right_1[s, :, here]
                right_3[s, :, here] = right_new
                twice = left_0[s, :, here]
                left_new = columns(left_1, left_1[s, :, here], s) + (up * left_new + down * left_1[s - step, :, here]) - (twice + twice)
                left_2[s, :, here] = left_new
            if levels >= 4:
                s = t - 4 * step
                up, down = toward(s)
                drift_3[s, :, here] = minus(up * right_new, down * right_3[s - step, :, here])
                left_new = columns(left_2, left_2[s, :, here], s) + (up * left_new + down * left_2[s - step, :, here]) - left_1[s, :, here]
                left_3[s, :, here] = left_new

    def multiply(s):
        product = None
        for lo in range(0, cols, CHUNK):
            here = pl.ds(lo, CHUNK)
            order_0 = split(left_0[s, :, here])
            lefts = jnp.concatenate([order_0] + [split(ref[s, :, here]) for ref in (left_1, left_2, left_3)], axis=0)
            drifts = jnp.concatenate([order_0] + [split(ref[s, :, here]) for ref in (drift_1, drift_2, drift_3)], axis=0)
            part = lax.dot_general(lefts, drifts, (((1,), (1,)), ((), ())), preferred_element_type=jnp.float32)
            product = part if product is None else product + part
        acc[...] += product

    for levels in range(4):

        def warm(t, carry, levels=levels):
            advance(t, levels)
            return carry

        lax.fori_loop(DEPTH + 2 * levels, DEPTH + 2 * levels + 2, warm, 0)
        if levels == 0:
            pl.when(crossing)(exchange)
        if levels == EXCHANGE_AT:
            pl.when(jnp.logical_not(jnp.logical_or(crossing, relaying)))(exchange)
        if levels == 3:
            pl.when(relaying)(exchange)
            pass_on(None, 0)

    first = 3 * DEPTH

    def inner(t, carry):
        @pl.when(t == first + 1)
        def _():
            acc[...] = jnp.zeros_like(acc)

        @pl.when(jnp.logical_and(relaying, t == RELAY_AT))
        def _():
            relay_on(0)

        @pl.when(jnp.logical_and(by_z, t == RELAY_AT))
        def _():
            relay_on(1)

        multiply(t - DEPTH - 1)
        advance(t, 4)
        return carry

    lax.fori_loop(first, rows + DEPTH, inner, 0)
    pass_on(0, 1)

    decode_side(0)
    for i in range(DEPTH):
        send_row(0, i).wait_recv()

    def near(k, carry):
        t = DEPTH - 1 - k
        multiply(t + DEPTH + 1 + (rows - 1 - 2 * DEPTH) * (t // (DEPTH - 1)))
        advance(t, 4, -1)
        return carry

    lax.fori_loop(0, DEPTH, near, 0)
    pass_on(1, 2)

    decode_side(1)

    def far(t, carry):
        pltpu.make_async_copy(signs.at[:, 0], raw.at[0], row_recv.at[1, t - (rows + DEPTH)]).wait()
        multiply(t - DEPTH - 1 - (rows - 1 - DEPTH) * ((total - 1 - t) // (DEPTH - 1)))
        advance(t, 4)
        return carry

    lax.fori_loop(rows + DEPTH, total, far, 0)
    pass_on(2, None)
    multiply(total - DEPTH - 1)

    whole = jnp.concatenate([acc[32 * b : 32 * b + 16, :] + acc[32 * b + 16 : 32 * b + 32, :] for b in range(4)], axis=0)
    whole = whole + rolled(whole, -16)
    lane = lax.broadcasted_iota(jnp.int32, (32, 128), 1)
    packed[...] = jnp.where((lane // 16) % 2 == 0, whole[:32], rolled(whole[32:], 16)).reshape(2, 16, 128)

    def send(src, dst, k, peer):
        return pltpu.make_async_remote_copy(
            src_ref=src, dst_ref=dst, send_sem=red_send.at[k], recv_sem=red_recv.at[k], device_id=peer, device_id_type=MESH
        )

    give = send(packed, core_in, 0, partner)
    take = send(final, final, 1, partner)

    @pl.when(summing)
    def _():
        give.wait_recv()
        halves = [packed[k] + core_in[k] for k in range(2)]
        waits = []
        start = 2
        places = (x * n_y + y, z)
        groups = (plane_peers, z_peers)
        for step in range(2):
            now = []
            for k in range(2):
                axis = (step + k) % 2
                buf = (plane_buf, z_buf)[axis].at[step]
                buf[places[axis]] = halves[k]
                for peer in groups[axis]:
                    now.append(send(buf.at[places[axis]], buf.at[places[axis]], start, peer))
                    now[-1].start()
                    start += 1
            for copy in now:
                copy.wait_recv()
            waits += now
            for k in range(2):
                axis = (step + k) % 2
                buf = (plane_buf, z_buf)[axis].at[step]
                value = buf[0]
                for j in range(1, len(groups[axis]) + 1):
                    value = value + buf[j]
                halves[k] = value
        for k in range(2):
            final[k] = halves[k]
        take.start()
        for copy in waits:
            copy.wait_send()

    @pl.when(jnp.logical_not(summing))
    def _():
        give.start()
        take.wait_recv()

    done = final[...].reshape(32, 128)
    per_site = -1.0 / (n_site * rows * cols * n_lo) / (scale * scale)
    for p in range(4):
        strip = done[(p % 2) * 16 : (p % 2) * 16 + 16]
        for q in range(4):
            block = rolled(strip, -(q * 32 + (p // 2) * 16))
            factor = per_site * (0.5 if p else 1.0) * (0.5 if q else 1.0)
            out[p, q] = block[:, :16] * factor

    @pl.when(summing)
    def _():
        take.wait_send()

    @pl.when(jnp.logical_not(summing))
    def _():
        give.wait_send()

    @pl.when(relaying)
    def _():
        for copy in relays(0):
            copy.wait_send()

    @pl.when(by_z)
    def _():
        for copy in relays(1):
            copy.wait_send()

    for side in range(2):
        for i in range(DEPTH):
            send_row(side, i).wait_send()
    for j in range(3):
        send_codes(True, j).wait_send()
    for i in range(DEPTH):
        send_far_codes(i).wait_send()


def solution(mesh):
    n_hi, n_x, n_y, n_core = SPLIT
    n_lo = mesh.shape["vec"]
    dims = (mesh.shape["site"] // (n_x * n_y * n_core), n_x, n_y, n_core, n_lo)

    def shards(vector_signs, disorder, bond_types, onsite_table, hop_table):
        width, rows, cols = vector_signs.shape
        total = rows + 2 * DEPTH
        n_z = dims[0] * n_lo
        n_red = 2 + 2 * (n_x * n_y - 1) + 2 * (n_z - 1)
        full = pltpu.VMEM((total, width, cols), jnp.float32)
        anywhere = pl.BlockSpec(memory_space=pl.ANY)
        scalars = pl.BlockSpec(memory_space=pltpu.SMEM)
        return pl.pallas_call(
            functools.partial(kernel, dims),
            out_shape=jax.ShapeDtypeStruct((4, 4, width, width), jnp.float32),
            in_specs=[anywhere, anywhere, anywhere, scalars, scalars],
            out_specs=pl.BlockSpec(memory_space=pltpu.VMEM),
            scratch_shapes=[
                pltpu.VMEM((3, total, cols), jnp.int32),
                pltpu.VMEM((3, total, 8, cols), jnp.float32),
                pltpu.VMEM((total + 1, 8, cols), jnp.float32),
                pltpu.VMEM((total, width, cols), jnp.int32),
                pltpu.VMEM((2, width, cols), jnp.int32),
                pltpu.VMEM((3, 2, cols), jnp.int32),
                full,
                full,
                full,
                full,
                full,
                full,
                full,
                full,
                full,
                full,
                full,
                pltpu.VMEM((128, 128), jnp.float32),
                pltpu.VMEM((2, 16, 128), jnp.float32),
                pltpu.VMEM((2, 16, 128), jnp.float32),
                pltpu.VMEM((2, n_x * n_y, 16, 128), jnp.float32),
                pltpu.VMEM((2, n_z, 16, 128), jnp.float32),
                pltpu.VMEM((2, 16, 128), jnp.float32),
                pltpu.SemaphoreType.DMA((rows,)),
                pltpu.SemaphoreType.DMA((3,)),
                pltpu.SemaphoreType.DMA((2, DEPTH)),
                pltpu.SemaphoreType.DMA((2, DEPTH)),
                pltpu.SemaphoreType.DMA((2, DEPTH)),
                pltpu.SemaphoreType.DMA((2, DEPTH)),
                pltpu.SemaphoreType.DMA((4, 2)),
                pltpu.SemaphoreType.REGULAR((3,)),
                pltpu.SemaphoreType.DMA((n_red,)),
                pltpu.SemaphoreType.DMA((n_red,)),
            ],
            compiler_params=pltpu.CompilerParams(
                collective_id=0, has_side_effects=True, vmem_limit_bytes=60 * 1024 * 1024
            ),
        )(vector_signs, disorder, bond_types, onsite_table, hop_table)

    return jax.shard_map(
        shards,
        mesh=mesh,
        in_specs=(P("vec", "site", None), P("site", None), P(None, "site", None), P(), P()),
        out_specs=P(),
        check_vma=False,
    )
```
